32 devices in a mesh: grp: 8 (over z, y), lane: 4 (over x, core).
Axes of the slice: x: 2, y: 2, z: 4, core: 2. Of those that a mesh axis runs over, the one named last changes fastest.
Arguments:
- grad_pooled: bfloat16 [4096, 16, 256], P(('grp', 'lane')), may hold values from -16 to 16
- bag_len: int32 [4096, 16], P(('grp', 'lane')), may hold values from 1 to 8
- lookup_slot: int32 [4096, 16, 8], P('grp', 'lane'), may hold values from -1 to 15, as said below
- slot_row: int32 [8, 4, 8, 2], P('grp', 'lane'), may hold values from 0 to 1023, as said below
- weights: float32 [16, 2048, 256], P('lane', 'grp'), may hold values from -6 to 6
- accum: float32 [16, 2048], P('lane', 'grp'), may hold values from 0.05 to 0.5
Outputs:
- new_weights: float32 [16, 2048, 256], P('lane', 'grp')
- new_accum: float32 [16, 2048], P('lane', 'grp')
The draws below stay inside these ranges and needn't reach their ends.
Inputs may be any that keep to these rules, and one draw needn't show every extreme that they name: `lookup_slot`: position j of bag (b, t) holds -1 when j >= bag_len[b, t] and otherwise a slot number s; the row slot_row[s // 2, t // 4, g, s % 2], with g the group of sample b, lies in local table t % 4. `slot_row`: several slots, also from different groups, may name the same row.
All inputs are finite; a program needn't handle non-finite values.
Results may differ from the reference program's by a relative error of at most 0.0035.
Values may be sent and summed in bfloat16 or wider, within the bound.
A program may use at most 64 MiB of HBM per device.

```python
import math
import jax
import jax.numpy as jnp
from jax import lax

EMBED = 256
TABLES_DEV = 4
BAG_MAX = 8
SLOTS_PEER = 2
BATCH_DEV = 128
ROWS_DEV = 256
TABLES = 16
BATCH = 4096
ROWS = 2048
SLOTS = 16
N_GRP = 8
N_LANE = 4
DEVICES = 32


def layout_keys(key):
    return jax.random.split(jax.random.fold_in(key, 913), 9)


def draw_grad_pooled(key, part):
    level_keys = jax.random.split(jax.random.fold_in(key, 421), 3)
    shape = (BATCH, TABLES, EMBED)
    level = jax.random.uniform(level_keys[0], (1, TABLES, 1), jnp.float32, -1.0, 1.0)
    base = 0.8 * jax.random.truncated_normal(level_keys[1], -4.0, 4.0, shape, jnp.float32)
    shared = 0.6 * jax.random.truncated_normal(level_keys[2], -3.0, 3.0, (1, TABLES, EMBED), jnp.float32)
    return ((base + shared) * jnp.exp(level)).astype(jnp.bfloat16)


def common_shift(key):
    keys = layout_keys(key)
    return jax.random.randint(keys[0], (N_LANE, N_GRP), 0, TABLES_DEV)


def common_lengths(key):
    keys = layout_keys(key)
    longest = jax.random.randint(keys[1], (DEVICES, 1, 1), 1, BAG_MAX + 1)
    raw_draw = jax.random.randint(keys[2], (DEVICES, BATCH_DEV, TABLES), 0, 1 << 20)
    lengths = (1 + raw_draw % longest).reshape(BATCH, TABLES)
    return lengths.at[0, 0].set(BAG_MAX).astype(jnp.int32)


def draw_bag_len(key, part):
    return common_lengths(key)


def draw_lookup_slot(key, part):
    keys = layout_keys(key)
    shift = common_shift(key)
    lengths = common_lengths(key)
    option_count = SLOTS // TABLES_DEV
    orders = jax.vmap(lambda one_key: jax.random.permutation(one_key, option_count))(jax.random.split(keys[3], N_LANE))
    shape = (BATCH, TABLES, BAG_MAX)
    first = jax.random.randint(keys[4], shape, 0, option_count)
    second = jax.random.randint(keys[5], shape, 0, option_count)
    third = jax.random.randint(keys[6], shape, 0, option_count)
    lowest = jnp.minimum(first, jnp.minimum(second, third))
    group_of = jnp.arange(BATCH, dtype=jnp.int32) // (BATCH_DEV * N_LANE)
    lane_of = jnp.arange(TABLES, dtype=jnp.int32) // TABLES_DEV
    table_local = jnp.arange(TABLES, dtype=jnp.int32) % TABLES_DEV
    picked = orders[lane_of[None, :, None], lowest]
    shift_here = shift[lane_of[None, :], group_of[:, None]]
    slot_number = picked * TABLES_DEV + ((table_local[None, :] - shift_here) % TABLES_DEV)[:, :, None]
    position = jnp.arange(BAG_MAX, dtype=jnp.int32)
    return jnp.where(position[None, None, :] < lengths[:, :, None], slot_number, -1).astype(jnp.int32)


def draw_slot_row(key, part):
    keys = layout_keys(key)
    shift = common_shift(key)
    slot_index = jnp.arange(SLOTS, dtype=jnp.int32).reshape(N_GRP, 1, 1, SLOTS_PEER)
    table_local = (slot_index + shift[None, :, :, None]) % TABLES_DEV
    shape = (N_GRP, N_LANE, N_GRP, SLOTS_PEER)
    hot_rows = jax.random.randint(keys[7], (N_GRP, N_LANE, 1, 8), 0, ROWS_DEV)
    sub_keys = jax.random.split(keys[8], 3)
    which = jax.random.randint(sub_keys[0], shape, 0, 8)
    hot_pick = jnp.take_along_axis(jnp.broadcast_to(hot_rows, (N_GRP, N_LANE, N_GRP, 8)), which, axis=3)
    drawn = jax.random.randint(sub_keys[1], shape, 0, ROWS_DEV)
    coin = jax.random.randint(sub_keys[2], shape, 0, 2)
    row_local = jnp.where(coin == 1, hot_pick, drawn)
    return (table_local * ROWS_DEV + row_local).astype(jnp.int32)


def block_levels(stream_key, shape, cuts, smallest, high):
    loudness, own = 1.0, jax.random.fold_in(stream_key, 6)
    for dim, parts in cuts:
        steps = jnp.exp(jax.random.uniform(jax.random.fold_in(own, dim), (parts,), jnp.float32, smallest / len(cuts), high / len(cuts)))
        loudness = loudness * jnp.repeat(steps, shape[dim] // parts).reshape([-1 if axis == dim else 1 for axis in range(len(shape))])
    return loudness


def noise(key, extent, width, bound, cuts=(), kind=jnp.bfloat16):
    values = jax.random.normal(key, extent, jnp.float32) * width
    if len(cuts) > 0:
        values = block_levels(key, extent, cuts, -0.22, 0.18) * values
    return jnp.clip(values, min=-bound, max=bound).astype(kind)


def setup_inputs(seed: int = 0) -> dict:
    seeds = jax.random.split(jax.random.key(seed), 7)
    grad_pooled = draw_grad_pooled(jax.random.fold_in(seeds[6], 71), 0)
    bag_len = draw_bag_len(jax.random.fold_in(seeds[6], 71), 0)
    lookup_slot = draw_lookup_slot(jax.random.fold_in(seeds[6], 71), 0)
    slot_row = draw_slot_row(jax.random.fold_in(seeds[6], 71), 0)
    weights = noise(seeds[4], (TABLES, ROWS, EMBED), 1.0, 6.0, ((0, 4), (1, 8)), jnp.float32)
    accum = jnp.clip(jnp.exp(math.log(0.5) - 2.3025851 * jax.random.uniform(seeds[5], (TABLES, ROWS), jnp.float32) ** block_levels(seeds[5], (TABLES, ROWS), ((0, 4), (1, 8)), -0.2, 0.2)), 0.05, 0.5)
    return {"grad_pooled": grad_pooled, "bag_len": bag_len, "lookup_slot": lookup_slot, "slot_row": slot_row, "weights": weights, "accum": accum}


def group_slot_sums(pieces):
    grad_block, length_block, slot_block = pieces
    scaled = (grad_block.astype(jnp.float32) / length_block.astype(jnp.float32)[:, :, None]).astype(jnp.bfloat16)
    values = scaled.astype(jnp.float32).reshape(N_LANE, BATCH_DEV, N_LANE, TABLES_DEV, 1, EMBED)
    slot_marks = slot_block.reshape(N_LANE, BATCH_DEV, N_LANE, TABLES_DEV, BAG_MAX)
    source_ids = jnp.arange(N_LANE, dtype=jnp.int32).reshape(N_LANE, 1, 1, 1, 1)
    target_ids = jnp.arange(N_LANE, dtype=jnp.int32).reshape(1, 1, N_LANE, 1, 1)
    dummy = N_LANE * N_LANE * SLOTS
    segment_ids = jnp.where(slot_marks >= 0, (source_ids * N_LANE + target_ids) * SLOTS + slot_marks, dummy)
    contrib = jnp.broadcast_to(values, (N_LANE, BATCH_DEV, N_LANE, TABLES_DEV, BAG_MAX, EMBED)).reshape(-1, EMBED)
    summed = jax.ops.segment_sum(contrib, segment_ids.reshape(-1).astype(jnp.int32), dummy + 1)
    partial_value = summed[:dummy].reshape(N_LANE, N_LANE, SLOTS, EMBED).astype(jnp.bfloat16)
    return lax.optimization_barrier(jnp.sum(partial_value.astype(jnp.float32), axis=0)).astype(jnp.bfloat16)

def reference(grad_pooled, bag_len, lookup_slot, slot_row, weights, accum):
    group_rows = N_LANE * BATCH_DEV
    slot_all = lax.map(group_slot_sums, (grad_pooled.reshape(N_GRP, group_rows, TABLES, EMBED), bag_len.reshape(N_GRP, group_rows, TABLES), lookup_slot.reshape(N_GRP, group_rows, TABLES, BAG_MAX)))
    local_index = jnp.transpose(slot_row, (2, 1, 0, 3))
    table_local = local_index // ROWS_DEV
    row_local = local_index % ROWS_DEV
    lane_ids = jnp.arange(N_LANE, dtype=jnp.int32).reshape(1, N_LANE, 1, 1)
    owner_ids = jnp.arange(N_GRP, dtype=jnp.int32).reshape(1, 1, N_GRP, 1)
    segment_ids = (lane_ids * TABLES_DEV + table_local) * ROWS + owner_ids * ROWS_DEV + row_local
    contrib = slot_all.astype(jnp.float32).reshape(-1, EMBED)
    row_grad = jax.ops.segment_sum(contrib, segment_ids.reshape(-1).astype(jnp.int32), TABLES * ROWS)
    row_grad = row_grad.reshape(TABLES, ROWS, EMBED)
    square_mean = lax.optimization_barrier(jnp.mean(row_grad * row_grad, axis=2))
    norm_total = EMBED * jnp.sum(square_mean)
    clip_limit = 0.5 * math.sqrt(DEVICES * SLOTS * EMBED)
    clip_factor = clip_limit / jnp.maximum(jnp.sqrt(norm_total), clip_limit)
    new_accum = accum + clip_factor * clip_factor * square_mean
    new_weights = weights - 0.3 * clip_factor * row_grad / (jnp.sqrt(new_accum)[:, :, None] + 1e-06)
    return (new_weights, new_accum)
```

```python
import functools
import math

import jax
import jax.numpy as jnp
from jax import lax
from jax.experimental import pallas as pl
from jax.experimental.pallas import tpu as pltpu
from jax.sharding import PartitionSpec as P

MESH = pl.DeviceIdType.MESH
LEARN_RATE = 0.3
EPSILON = 1e-06
F32 = jnp.float32
BF16 = jnp.bfloat16


def each(count, body):
    if count <= 64:
        for i in range(count):
            body(i)
    else:

        def step(i, carry):
            body(i)
            return carry

        lax.fori_loop(0, count, step, 0)


def iota(shape, dim):
    return lax.broadcasted_iota(jnp.int32, shape, dim)


def kernel(
    groups,
    lanes,
    grad_hbm,
    len_hbm,
    look_hbm,
    slot_hbm,
    weights_hbm,
    accum_hbm,
    wout,
    aout,
    grad_in,
    grad_f32,
    grad_t,
    len_v,
    marks,
    marks_out,
    slot_v,
    accum_v,
    part,
    recv,
    incoming,
    norm_out,
    norm_in,
    load_sem,
    look_sem,
    a_send,
    a_recv,
    b_send,
    b_recv,
    c_send,
    c_recv,
):
    devices = groups * lanes
    per_peer, embed = recv.shape[1], recv.shape[2]
    slots = groups * per_peer
    tables_all, batch = grad_t.shape[0], grad_t.shape[1]
    tables = tables_all // lanes
    depth = marks.shape[2]
    rows = accum_v.shape[1]
    grp = lax.axis_index("grp")
    lane = lax.axis_index("lane")
    me = grp * lanes + lane

    lane_steps = [(dx, dc) for dx in range(lanes // 2) for dc in range(2)]

    def lane_peer(step, sign):
        dx, dc = step
        half = lanes // 2
        chip = (lane // 2 + sign * dx + half) % half
        return chip * 2 + (lane % 2 + dc) % 2

    barrier = pltpu.get_barrier_semaphore()

    def greet(i):
        far = (me + i + 1) % devices
        pl.semaphore_signal(
            barrier, inc=1, device_id=(far // lanes, far % lanes), device_id_type=MESH
        )

    look_copies = []
    for k, step in enumerate(lane_steps):
        q = lane_peer(step, 1)
        src = look_hbm.at[:, :, pl.ds(pl.multiple_of(q * batch, batch), batch)]
        dst = marks.at[lane] if k == 0 else marks_out.at[k - 1]
        look_copies.append(pltpu.make_async_copy(src, dst, look_sem.at[k]))
        look_copies[-1].start()
    grad_copy = pltpu.make_async_copy(grad_hbm, grad_in, load_sem.at[0])
    grad_copy.start()
    each(devices - 1, greet)
    small_copies = [
        pltpu.make_async_copy(len_hbm, len_v, load_sem.at[1]),
        pltpu.make_async_copy(slot_hbm, slot_v, load_sem.at[2]),
        pltpu.make_async_copy(accum_hbm, accum_v, load_sem.at[3]),
        pltpu.make_async_copy(weights_hbm, wout, load_sem.at[4]),
    ]
    for copy in small_copies:
        copy.start()
    for copy in look_copies:
        copy.wait()
    pl.semaphore_wait(barrier, devices - 1)

    a_copies = []
    for k, step in enumerate(lane_steps[1:], 1):
        copy = pltpu.make_async_remote_copy(
            src_ref=marks_out.at[k - 1],
            dst_ref=marks.at[lane],
            send_sem=a_send.at[k - 1],
            recv_sem=a_recv.at[k - 1],
            device_id=(grp, lane_peer(step, 1)),
            device_id_type=MESH,
        )
        copy.start()
        a_copies.append(copy)

    grad_copy.wait()
    for c in range(embed // 128):
        grad_f32[c] = grad_in[:, c * 128 : (c + 1) * 128].astype(F32)
    for t in range(tables_all):
        for c in range(embed // 128):
            grad_t[t, :, c * 128 : (c + 1) * 128] = grad_f32[
                c, pl.ds(t, batch, stride=tables_all), :
            ].astype(BF16)
    for copy in small_copies[:3]:
        copy.wait()

    number = iota((slots, batch), 0)
    far_first = sorted(range(groups), key=lambda d: abs(d - groups // 2))

    for k, step in enumerate(lane_steps):
        m = lane_peer(step, -1)
        if k > 0:
            a_copies[k - 1].wait_recv()
        highs, lows = [], []
        for t in range(tables):
            mark = marks[m, t]
            count = jnp.zeros((slots, batch), F32)
            for j in range(depth):
                count += jnp.where(mark[j : j + 1, :] == number, 1.0, 0.0)
            length = len_v[pl.ds(m * tables + t, 1), :].astype(F32)
            factor = count / length
            high = factor.astype(BF16)
            highs.append(high)
            lows.append((factor - high.astype(F32)).astype(BF16))
        factors = jnp.concatenate(
            [jnp.concatenate(highs, axis=1), jnp.concatenate(lows, axis=1)], axis=0
        )
        values = grad_t[pl.ds(m * tables, tables)].reshape(tables * batch, embed)
        both = jnp.dot(factors, values, preferred_element_type=F32)
        total = both[:slots] + both[slots:]
        for p in range(groups):
            part[m, p] = total[p * per_peer : (p + 1) * per_peer].astype(BF16)

        def send(p):
            pltpu.make_async_remote_copy(
                src_ref=part.at[m, p],
                dst_ref=recv.at[me],
                send_sem=b_send,
                recv_sem=b_recv,
                device_id=(p, m),
                device_id_type=MESH,
            ).start()

        if groups <= 64:
            for dp in far_first:
                if k == 0 and dp == 0:
                    pltpu.make_async_copy(part.at[m, grp], recv.at[me], b_recv).start()
                else:
                    send((grp + dp) % groups)
        else:
            each(groups - 1, lambda i: send((grp + i + 1) % groups))
            if k == 0:
                pltpu.make_async_copy(part.at[m, grp], recv.at[me], b_recv).start()
            else:
                send(grp)

    slot_f = slot_v[...].astype(F32)
    which = iota((slots, groups), 0)
    column_pick = jnp.zeros((slots, groups), F32)
    for k in range(per_peer):
        column_pick = jnp.where(which % per_peer == k, slot_f[k : k + 1, :], column_pick)
    column_pick = jnp.where(which // per_peer == iota((slots, groups), 1), column_pick, 0.0)
    target_col = jnp.sum(column_pick, axis=1, keepdims=True)
    i_id, j_id = iota((slots, slots), 0), iota((slots, slots), 1)
    target_row = jnp.sum(jnp.where(i_id == j_id, target_col, 0.0), axis=0, keepdims=True)
    same = target_col == target_row
    first_col = jnp.sum(jnp.where(same & (j_id < i_id), 1.0, 0.0), axis=1, keepdims=True) == 0.0
    first_row = jnp.sum(jnp.where(same & (i_id < j_id), 1.0, 0.0), axis=0, keepdims=True) == 0.0
    place_row = jnp.where(first_row, target_row, -1.0)
    place_row = jnp.concatenate([place_row, place_row], axis=1)
    same_w = jnp.where(same, 1.0, 0.0).astype(BF16)

    hits = []
    accum_col = jnp.zeros((slots, 1), F32)
    for t in range(tables):
        hit = target_col == (iota((slots, rows), 1) + t * rows).astype(F32)
        hits.append(hit)
        accum_col += jnp.sum(
            jnp.where(hit, accum_v[t : t + 1, :], 0.0), axis=1, keepdims=True
        )

    pltpu.make_async_copy(recv, recv, b_recv).wait()
    for g in range(groups):
        group_sum = recv[g * lanes].astype(F32)
        for q in range(1, lanes):
            group_sum += recv[g * lanes + q].astype(F32)
        incoming[g * per_peer : (g + 1) * per_peer, :] = group_sum
    grads = jnp.dot(same_w, incoming[...].astype(BF16), preferred_element_type=F32)
    square_col = jnp.sum(grads * grads, axis=1, keepdims=True) * (1.0 / embed)
    square_first = jnp.where(first_col, square_col, 0.0)
    local = embed * jnp.sum(square_first, axis=0, keepdims=True)
    norm_out[...] = jnp.broadcast_to(local, (1, 128))

    def tell(far):
        pltpu.make_async_remote_copy(
            src_ref=norm_out,
            dst_ref=norm_in.at[me],
            send_sem=c_send,
            recv_sem=c_recv,
            device_id=(far // lanes, far % lanes),
            device_id_type=MESH,
        ).start()

    if devices <= 64:
        for d in sorted(range(1, devices), key=lambda d: abs(d - devices // 2)):
            tell((me + d) % devices)
    else:
        each(devices - 1, lambda i: tell((me + i + 1) % devices))
    pltpu.make_async_copy(norm_out, norm_in.at[me], c_recv).start()

    square_rows = [
        jnp.sum(jnp.where(hit, square_first, 0.0), axis=0, keepdims=True) for hit in hits
    ]
    for copy in a_copies:
        copy.wait_send()
    small_copies[3].wait()
    sent = recv.at[pl.ds(0, devices - 1)]
    pltpu.make_async_copy(sent, sent, b_send).wait()

    pltpu.make_async_copy(norm_in, norm_in, c_recv).wait()
    norm_total = jnp.sum(norm_in[...], axis=0)[:, :1]
    clip_limit = 0.5 * math.sqrt(devices * slots * embed)
    clip = clip_limit / jnp.maximum(jnp.sqrt(norm_total), clip_limit)
    for t in range(tables):
        aout[t : t + 1, :] = accum_v[t : t + 1, :] + clip * clip * square_rows[t]
    new_accum_col = accum_col + clip * clip * square_col
    delta = LEARN_RATE * clip * grads / (jnp.sqrt(new_accum_col) + EPSILON)
    delta_high = delta.astype(BF16)
    delta_low = (delta - delta_high.astype(F32)).astype(BF16)
    deltas = jnp.concatenate([delta_high, delta_low], axis=0)
    for t in range(tables):
        row_id = (iota((rows, 1), 0) + t * rows).astype(F32)
        place = jnp.where(row_id == place_row, 1.0, 0.0).astype(BF16)
        wout[t] = wout[t] - jnp.dot(place, deltas, preferred_element_type=F32)
    told = norm_in.at[pl.ds(0, devices - 1)]
    pltpu.make_async_copy(told, told, c_send).wait()


def per_device(groups, lanes, grad_pooled, bag_len, lookup_slot, slot_row, weights, accum):
    batch, tables_all, embed = grad_pooled.shape
    samples, tables, depth = lookup_slot.shape
    rows = accum.shape[1]
    per_peer = slot_row.shape[3]
    devices = groups * lanes
    slots = groups * per_peer
    anywhere = pl.BlockSpec(memory_space=pl.ANY)
    vmem = pl.BlockSpec(memory_space=pltpu.VMEM)
    return pl.pallas_call(
        functools.partial(kernel, groups, lanes),
        out_shape=(
            jax.ShapeDtypeStruct(weights.shape, F32),
            jax.ShapeDtypeStruct(accum.shape, F32),
        ),
        in_specs=[anywhere] * 6,
        out_specs=(vmem, vmem),
        scratch_shapes=[
            pltpu.VMEM((batch * tables_all, embed), BF16),
            pltpu.VMEM((embed // 128, batch * tables_all, 128), F32),
            pltpu.VMEM((tables_all, batch, embed), BF16),
            pltpu.VMEM((tables_all, batch), jnp.int32),
            pltpu.VMEM((lanes, tables, depth, batch), jnp.int32),
            pltpu.VMEM((lanes - 1, tables, depth, batch), jnp.int32),
            pltpu.VMEM((per_peer, groups), jnp.int32),
            pltpu.VMEM((tables, rows), F32),
            pltpu.VMEM((lanes, groups, per_peer, embed), BF16),
            pltpu.VMEM((devices, per_peer, embed), BF16),
            pltpu.VMEM((slots, embed), F32),
            pltpu.VMEM((1, 128), F32),
            pltpu.VMEM((devices, 1, 128), F32),
            pltpu.SemaphoreType.DMA((5,)),
            pltpu.SemaphoreType.DMA((lanes,)),
            pltpu.SemaphoreType.DMA((lanes - 1,)),
            pltpu.SemaphoreType.DMA((lanes - 1,)),
            pltpu.SemaphoreType.DMA,
            pltpu.SemaphoreType.DMA,
            pltpu.SemaphoreType.DMA,
            pltpu.SemaphoreType.DMA,
        ],
        compiler_params=pltpu.CompilerParams(collective_id=0, has_side_effects=True),
    )(
        grad_pooled.reshape(batch * tables_all, embed),
        bag_len.T,
        jnp.transpose(lookup_slot, (1, 2, 0)),
        slot_row.reshape(groups, per_peer).T,
        weights,
        accum,
    )


def solution(mesh):
    placed = (
        P(("grp", "lane"), None, None),
        P(("grp", "lane"), None),
        P("grp", "lane", None),
        P("grp", "lane", None, None),
        P("lane", "grp", None),
        P("lane", "grp"),
    )
    return jax.shard_map(
        functools.partial(per_device, mesh.shape["grp"], mesh.shape["lane"]),
        mesh=mesh,
        in_specs=placed,
        out_specs=(P("lane", "grp", None), P("lane", "grp")),
        check_vma=False,
    )
```

```python
import functools
import math

import jax
import jax.numpy as jnp
from jax import lax
from jax.experimental import pallas as pl
from jax.experimental.pallas import tpu as pltpu
from jax.sharding import PartitionSpec as P

MESH = pl.DeviceIdType.MESH
LEARN_RATE = 0.3
EPSILON = 1e-06
F32 = jnp.float32
BF16 = jnp.bfloat16


def each(count, body):
    if count <= 64:
        for i in range(count):
            body(i)
    else:

        def step(i, carry):
            body(i)
            return carry

        lax.fori_loop(0, count, step, 0)


def iota(shape, dim):
    return lax.broadcasted_iota(jnp.int32, shape, dim)


def kernel(
    groups,
    lanes,
    grad_hbm,
    len_hbm,
    look_hbm,
    slot_hbm,
    accum_hbm,
    delta_out,
    place_out,
    aout,
    grad_in,
    grad_f32,
    grad_t,
    len_v,
    marks,
    marks_out,
    slot_v,
    accum_v,
    part,
    recv,
    incoming,
    norm_out,
    norm_in,
    load_sem,
    look_sem,
    a_send,
    a_recv,
    b_send,
    b_recv,
    c_send,
    c_recv,
):
    devices = groups * lanes
    per_peer, embed = recv.shape[1], recv.shape[2]
    slots = groups * per_peer
    tables_all, batch = grad_t.shape[0], grad_t.shape[1]
    tables = tables_all // lanes
    depth = marks.shape[2]
    rows = accum_v.shape[1]
    grp = lax.axis_index("grp")
    lane = lax.axis_index("lane")
    me = grp * lanes + lane

    lane_steps = [(dx, dc) for dx in range(lanes // 2) for dc in range(2)]

    def lane_peer(step, sign):
        dx, dc = step
        half = lanes // 2
        chip = (lane // 2 + sign * dx + half) % half
        return chip * 2 + (lane % 2 + dc) % 2

    def partial_of(m):
        highs, lows = [], []
        for t in range(tables):
            mark = marks[m, t]
            count = jnp.zeros((slots, batch), F32)
            for j in range(depth):
                count += jnp.where(mark[j : j + 1, :] == number, 1.0, 0.0)
            length = len_v[pl.ds(m * tables + t, 1), :].astype(F32)
            factor = count / length
            high = factor.astype(BF16)
            highs.append(high)
            lows.append((factor - high.astype(F32)).astype(BF16))
        factors = jnp.concatenate(
            [jnp.concatenate(highs, axis=1), jnp.concatenate(lows, axis=1)], axis=0
        )
        values = grad_t[pl.ds(m * tables, tables)].reshape(tables * batch, embed)
        both = jnp.dot(factors, values, preferred_element_type=F32)
        return both[:slots] + both[slots:]

    barrier = pltpu.get_barrier_semaphore()

    def greet(i):
        far = (me + i + 1) % devices
        pl.semaphore_signal(
            barrier, inc=1, device_id=(far // lanes, far % lanes), device_id_type=MESH
        )

    if devices <= 64:
        for i in sorted(range(devices - 1), key=lambda i: abs(i + 1 - devices // 2)):
            greet(i)
    else:
        each(devices - 1, greet)
    look_copies = []
    for k, step in enumerate(lane_steps):
        q = lane_peer(step, 1)
        src = look_hbm.at[:, :, pl.ds(pl.multiple_of(q * batch, batch), batch)]
        dst = marks.at[lane] if k == 0 else marks_out.at[k - 1]
        look_copies.append(pltpu.make_async_copy(src, dst, look_sem.at[k]))
        look_copies[-1].start()
    grad_copy = pltpu.make_async_copy(grad_hbm, grad_in, load_sem.at[0])
    grad_copy.start()
    small_copies = [
        pltpu.make_async_copy(len_hbm, len_v, load_sem.at[1]),
        pltpu.make_async_copy(slot_hbm, slot_v, load_sem.at[2]),
        pltpu.make_async_copy(accum_hbm, accum_v, load_sem.at[3]),
    ]
    for copy in small_copies:
        copy.start()
    for copy in look_copies:
        copy.wait()
    grad_copy.wait()
    for c in range(embed // 128):
        grad_f32[c] = grad_in[:, c * 128 : (c + 1) * 128].astype(F32)
    for t in range(tables_all):
        for c in range(embed // 128):
            grad_t[t, :, c * 128 : (c + 1) * 128] = grad_f32[
                c, pl.ds(t, batch, stride=tables_all), :
            ].astype(BF16)
    for copy in small_copies:
        copy.wait()

    number = iota((slots, batch), 0)
    own_part = partial_of(lane)
    pl.semaphore_wait(barrier, devices - 1)

    a_copies = []
    for k, step in enumerate(lane_steps[1:], 1):
        copy = pltpu.make_async_remote_copy(
            src_ref=marks_out.at[k - 1],
            dst_ref=marks.at[lane],
            send_sem=a_send.at[k - 1],
            recv_sem=a_recv.at[k - 1],
            device_id=(grp, lane_peer(step, 1)),
            device_id_type=MESH,
        )
        copy.start()
        a_copies.append(copy)

    far_first = sorted(range(groups), key=lambda d: abs(d - groups // 2))

    for k, step in enumerate(lane_steps):
        m = lane_peer(step, -1)
        if k > 0:
            a_copies[k - 1].wait_recv()
        total = own_part if k == 0 else partial_of(m)
        for p in range(groups):
            part[m, p] = total[p * per_peer : (p + 1) * per_peer].astype(BF16)

        def send(p):
            pltpu.make_async_remote_copy(
                src_ref=part.at[m, p],
                dst_ref=recv.at[me],
                send_sem=b_send,
                recv_sem=b_recv,
                device_id=(p, m),
                device_id_type=MESH,
            ).start()

        if groups <= 64:
            for dp in far_first:
                if k == 0 and dp == 0:
                    pltpu.make_async_copy(part.at[m, grp], recv.at[me], b_recv).start()
                else:
                    send((grp + dp) % groups)
        else:
            each(groups - 1, lambda i: send((grp + i + 1) % groups))
            if k == 0:
                pltpu.make_async_copy(part.at[m, grp], recv.at[me], b_recv).start()
            else:
                send(grp)

    slot_f = slot_v[...].astype(F32)
    which = iota((slots, groups), 0)
    column_pick = jnp.zeros((slots, groups), F32)
    for k in range(per_peer):
        column_pick = jnp.where(which % per_peer == k, slot_f[k : k + 1, :], column_pick)
    column_pick = jnp.where(which // per_peer == iota((slots, groups), 1), column_pick, 0.0)
    target_col = jnp.sum(column_pick, axis=1, keepdims=True)
    i_id, j_id = iota((slots, slots), 0), iota((slots, slots), 1)
    target_row = jnp.sum(jnp.where(i_id == j_id, target_col, 0.0), axis=0, keepdims=True)
    same = target_col == target_row
    first_col = jnp.sum(jnp.where(same & (j_id < i_id), 1.0, 0.0), axis=1, keepdims=True) == 0.0
    first_row = jnp.sum(jnp.where(same & (i_id < j_id), 1.0, 0.0), axis=0, keepdims=True) == 0.0
    place_row = jnp.where(first_row, target_row, -1.0)
    place_out[...] = jnp.concatenate([place_row, place_row], axis=1)
    same_w = jnp.where(same, 1.0, 0.0).astype(BF16)

    hits = []
    accum_col = jnp.zeros((slots, 1), F32)
    for t in range(tables):
        hit = target_col == (iota((slots, rows), 1) + t * rows).astype(F32)
        hits.append(hit)
        accum_col += jnp.sum(
            jnp.where(hit, accum_v[t : t + 1, :], 0.0), axis=1, keepdims=True
        )

    pltpu.make_async_copy(recv, recv, b_recv).wait()
    for g in range(groups):
        group_sum = recv[g * lanes].astype(F32)
        for q in range(1, lanes):
            group_sum += recv[g * lanes + q].astype(F32)
        incoming[g * per_peer : (g + 1) * per_peer, :] = group_sum
    grads = jnp.dot(same_w, incoming[...].astype(BF16), preferred_element_type=F32)
    square_col = jnp.sum(grads * grads, axis=1, keepdims=True) * (1.0 / embed)
    square_first = jnp.where(first_col, square_col, 0.0)
    local = embed * jnp.sum(square_first, axis=0, keepdims=True)
    norm_out[...] = jnp.broadcast_to(local, (1, 128))

    def tell(far):
        pltpu.make_async_remote_copy(
            src_ref=norm_out,
            dst_ref=norm_in.at[me],
            send_sem=c_send,
            recv_sem=c_recv,
            device_id=(far // lanes, far % lanes),
            device_id_type=MESH,
        ).start()

    if devices <= 64:
        for d in sorted(range(1, devices), key=lambda d: abs(d - devices // 2)):
            tell((me + d) % devices)
    else:
        each(devices - 1, lambda i: tell((me + i + 1) % devices))
    pltpu.make_async_copy(norm_out, norm_in.at[me], c_recv).start()

    square_rows = [
        jnp.sum(jnp.where(hit, square_first, 0.0), axis=0, keepdims=True) for hit in hits
    ]
    for copy in a_copies:
        copy.wait_send()
    sent = recv.at[pl.ds(0, devices - 1)]
    pltpu.make_async_copy(sent, sent, b_send).wait()

    pltpu.make_async_copy(norm_in, norm_in, c_recv).wait()
    norm_total = jnp.sum(norm_in[...], axis=0)[:, :1]
    clip_limit = 0.5 * math.sqrt(devices * slots * embed)
    clip = clip_limit / jnp.maximum(jnp.sqrt(norm_total), clip_limit)
    for t in range(tables):
        aout[t : t + 1, :] = accum_v[t : t + 1, :] + clip * clip * square_rows[t]
    new_accum_col = accum_col + clip * clip * square_col
    delta = LEARN_RATE * clip * grads / (jnp.sqrt(new_accum_col) + EPSILON)
    delta_high = delta.astype(BF16)
    delta_out[:slots] = delta_high
    delta_out[slots:] = (delta - delta_high.astype(F32)).astype(BF16)
    told = norm_in.at[pl.ds(0, devices - 1)]
    pltpu.make_async_copy(told, told, c_send).wait()


def update_kernel(
    chunk,
    weights,
    delta_any,
    place_any,
    accum_any,
    wout,
    aout,
    held,
    delta,
    place_row,
    accum,
    sems,
    in_sems,
    accum_sem,
):
    loads = [
        pltpu.make_async_copy(place_any, place_row, in_sems.at[0]),
        pltpu.make_async_copy(delta_any, delta, in_sems.at[1]),
        pltpu.make_async_copy(accum_any, accum, in_sems.at[2]),
    ]
    for copy in loads:
        copy.start()
    for copy in loads:
        copy.wait()
    accum_copy = pltpu.make_async_copy(accum, aout, accum_sem)
    accum_copy.start()
    tables, rows = weights.shape[0], weights.shape[1]
    copies = []
    for t in range(tables):
        for c in range(0, rows, chunk):
            row_id = (iota((chunk, 1), 0) + (t * rows + c)).astype(F32)
            place = jnp.where(row_id == place_row[...], 1.0, 0.0).astype(BF16)
            held[t, c : c + chunk] = weights[t, c : c + chunk] - jnp.dot(
                place, delta[...], preferred_element_type=F32
            )
            copies.append(
                pltpu.make_async_copy(
                    held.at[t, pl.ds(c, chunk)],
                    wout.at[t, pl.ds(c, chunk)],
                    sems.at[len(copies)],
                )
            )
            copies[-1].start()
    for copy in copies:
        copy.wait()
    accum_copy.wait()


def per_device(groups, lanes, grad_pooled, bag_len, lookup_slot, slot_row, weights, accum):
    batch, tables_all, embed = grad_pooled.shape
    samples, tables, depth = lookup_slot.shape
    rows = accum.shape[1]
    per_peer = slot_row.shape[3]
    devices = groups * lanes
    slots = groups * per_peer
    anywhere = pl.BlockSpec(memory_space=pl.ANY)
    vmem = pl.BlockSpec(memory_space=pltpu.VMEM)
    delta, place_row, accum_new = pl.pallas_call(
        functools.partial(kernel, groups, lanes),
        out_shape=(
            jax.ShapeDtypeStruct((2 * slots, embed), BF16),
            jax.ShapeDtypeStruct((1, 2 * slots), F32),
            jax.ShapeDtypeStruct(accum.shape, F32),
        ),
        in_specs=[pl.BlockSpec(memory_space=pltpu.HBM)] * 5,
        out_specs=(vmem, vmem, vmem),
        cost_estimate=pl.CostEstimate(
            flops=8 * slots * batch * tables_all * embed,
            bytes_accessed=32 * batch * tables_all * embed,
            transcendentals=0,
        ),
        scratch_shapes=[
            pltpu.VMEM((batch * tables_all, embed), BF16),
            pltpu.VMEM((embed // 128, batch * tables_all, 128), F32),
            pltpu.VMEM((tables_all, batch, embed), BF16),
            pltpu.VMEM((tables_all, batch), jnp.int32),
            pltpu.VMEM((lanes, tables, depth, batch), jnp.int32),
            pltpu.VMEM((lanes - 1, tables, depth, batch), jnp.int32),
            pltpu.VMEM((per_peer, groups), jnp.int32),
            pltpu.VMEM((tables, rows), F32),
            pltpu.VMEM((lanes, groups, per_peer, embed), BF16),
            pltpu.VMEM((devices, per_peer, embed), BF16),
            pltpu.VMEM((slots, embed), F32),
            pltpu.VMEM((1, 128), F32),
            pltpu.VMEM((devices, 1, 128), F32),
            pltpu.SemaphoreType.DMA((4,)),
            pltpu.SemaphoreType.DMA((lanes,)),
            pltpu.SemaphoreType.DMA((lanes - 1,)),
            pltpu.SemaphoreType.DMA((lanes - 1,)),
            pltpu.SemaphoreType.DMA,
            pltpu.SemaphoreType.DMA,
            pltpu.SemaphoreType.DMA,
            pltpu.SemaphoreType.DMA,
        ],
        compiler_params=pltpu.CompilerParams(
            collective_id=0, has_side_effects=True
        ),
    )(
        grad_pooled.reshape(batch * tables_all, embed),
        bag_len.T,
        jnp.transpose(lookup_slot, (1, 2, 0)),
        slot_row.reshape(groups, per_peer).T,
        accum,
    )
    chunk = min(rows, 128)
    return pl.pallas_call(
        functools.partial(update_kernel, chunk),
        out_shape=(
            jax.ShapeDtypeStruct(weights.shape, F32),
            jax.ShapeDtypeStruct(accum.shape, F32),
        ),
        in_specs=[vmem, anywhere, anywhere, anywhere],
        out_specs=(anywhere, anywhere),
        scratch_shapes=[
            pltpu.VMEM(weights.shape, F32),
            pltpu.VMEM(delta.shape, BF16),
            pltpu.VMEM(place_row.shape, F32),
            pltpu.VMEM(accum.shape, F32),
            pltpu.SemaphoreType.DMA((tables * (rows // chunk),)),
            pltpu.SemaphoreType.DMA((3,)),
            pltpu.SemaphoreType.DMA,
        ],
        compiler_params=pltpu.CompilerParams(vmem_limit_bytes=8 << 20),
    )(weights, delta, place_row, accum_new)


def solution(mesh):
    placed = (
        P(("grp", "lane"), None, None),
        P(("grp", "lane"), None),
        P("grp", "lane", None),
        P("grp", "lane", None, None),
        P("lane", "grp", None),
        P("lane", "grp"),
    )
    return jax.shard_map(
        functools.partial(per_device, mesh.shape["grp"], mesh.shape["lane"]),
        mesh=mesh,
        in_specs=placed,
        out_specs=(P("lane", "grp", None), P("lane", "grp")),
        check_vma=False,
    )
```

```python
import functools
import math

import jax
import jax.numpy as jnp
from jax import lax
from jax.experimental import pallas as pl
from jax.experimental.pallas import tpu as pltpu
from jax.sharding import PartitionSpec as P

MESH = pl.DeviceIdType.MESH
LEARN_RATE = 0.3
EPSILON = 1e-06
F32 = jnp.float32
BF16 = jnp.bfloat16


def each(count, body):
    if count <= 64:
        for i in range(count):
            body(i)
    else:

        def step(i, carry):
            body(i)
            return carry

        lax.fori_loop(0, count, step, 0)


def iota(shape, dim):
    return lax.broadcasted_iota(jnp.int32, shape, dim)


def kernel(
    groups,
    lanes,
    place_base,
    accum_base,
    grad_hbm,
    len_hbm,
    look_hbm,
    slot_hbm,
    accum_hbm,
    packed,
    grad_in,
    grad_f32,
    grad_t,
    len_v,
    marks,
    marks_in,
    marks_out,
    slot_v,
    accum_v,
    part,
    recv,
    incoming,
    norm_out,
    norm_in,
    load_sem,
    look_sem,
    a_send,
    a_recv,
    b_send,
    b_recv,
    c_send,
    c_recv,
):
    devices = groups * lanes
    per_peer, embed = recv.shape[1], recv.shape[2]
    slots = groups * per_peer
    tables_all, batch = grad_t.shape[0], grad_t.shape[1]
    tables = tables_all // lanes
    depth = marks.shape[2]
    rows = accum_v.shape[1]
    grp = lax.axis_index("grp")
    lane = lax.axis_index("lane")
    me = grp * lanes + lane

    lane_steps = [(dx, dc) for dx in range(lanes // 2) for dc in range(2)]

    def lane_peer(step, sign):
        dx, dc = step
        half = lanes // 2
        chip = (lane // 2 + sign * dx + half) % half
        return chip * 2 + (lane % 2 + dc) % 2

    def partial_of(m):
        highs, lows = [], []
        for t in range(tables):
            mark = marks[m, t].astype(F32)
            count = jnp.zeros((slots, batch), F32)
            for j in range(depth):
                count += jnp.where(mark[j : j + 1, :] == number, 1.0, 0.0)
            length = len_v[pl.ds(m * tables + t, 1), :].astype(F32)
            factor = count / length
            high = factor.astype(BF16)
            highs.append(high)
            lows.append((factor - high.astype(F32)).astype(BF16))
        factors = jnp.concatenate(
            [jnp.concatenate(highs, axis=1), jnp.concatenate(lows, axis=1)], axis=0
        )
        values = grad_t[pl.ds(m * tables, tables)].reshape(tables * batch, embed)
        both = jnp.dot(factors, values, preferred_element_type=F32)
        return both[:slots] + both[slots:]

    barrier = pltpu.get_barrier_semaphore()

    def greet(i):
        far = (me + i + 1) % devices
        pl.semaphore_signal(
            barrier, inc=1, device_id=(far // lanes, far % lanes), device_id_type=MESH
        )

    look_copies = []
    for k, step in enumerate(lane_steps):
        q = lane_peer(step, 1)
        src = look_hbm.at[:, :, pl.ds(pl.multiple_of(q * batch, batch), batch)]
        look_copies.append(pltpu.make_async_copy(src, marks_in.at[k], look_sem.at[k]))
        look_copies[-1].start()
    grad_copy = pltpu.make_async_copy(grad_hbm, grad_in, load_sem.at[0])
    grad_copy.start()
    if devices <= 64:
        for i in sorted(range(devices - 1), key=lambda i: abs(i + 1 - devices // 2)):
            greet(i)
    else:
        each(devices - 1, greet)
    small_copies = [
        pltpu.make_async_copy(len_hbm, len_v, load_sem.at[1]),
        pltpu.make_async_copy(slot_hbm, slot_v, load_sem.at[2]),
        pltpu.make_async_copy(accum_hbm, accum_v, load_sem.at[3]),
    ]
    for copy in small_copies:
        copy.start()
    for copy in look_copies:
        copy.wait()
    for k in range(1, lanes):
        marks_out[k - 1] = marks_in[k].astype(F32).astype(marks_out.dtype)
    pl.semaphore_wait(barrier, devices - 1)

    a_copies = []
    for k, step in enumerate(lane_steps[1:], 1):
        copy = pltpu.make_async_remote_copy(
            src_ref=marks_out.at[k - 1],
            dst_ref=marks.at[lane],
            send_sem=a_send.at[k - 1],
            recv_sem=a_recv.at[k - 1],
            device_id=(grp, lane_peer(step, 1)),
            device_id_type=MESH,
        )
        copy.start()
        a_copies.append(copy)

    grad_copy.wait()
    for c in range(embed // 128):
        grad_f32[c] = grad_in[:, c * 128 : (c + 1) * 128].astype(F32)
    for t in range(tables_all):
        for c in range(embed // 128):
            grad_t[t, :, c * 128 : (c + 1) * 128] = grad_f32[
                c, pl.ds(t, batch, stride=tables_all), :
            ].astype(BF16)
    for copy in small_copies:
        copy.wait()

    marks[lane] = marks_in[0].astype(F32).astype(marks.dtype)
    number = iota((slots, batch), 0).astype(F32)
    far_first = sorted(range(groups), key=lambda d: abs(d - groups // 2))

    for k, step in enumerate(lane_steps):
        m = lane_peer(step, -1)
        if k > 0:
            a_copies[k - 1].wait_recv()
        total = partial_of(m)
        for p in range(groups):
            part[m, p] = total[p * per_peer : (p + 1) * per_peer].astype(BF16)

        def send(p):
            pltpu.make_async_remote_copy(
                src_ref=part.at[m, p],
                dst_ref=recv.at[me],
                send_sem=b_send,
                recv_sem=b_recv,
                device_id=(p, m),
                device_id_type=MESH,
            ).start()

        if groups <= 64:
            for dp in far_first:
                if k == 0 and dp == 0:
                    pltpu.make_async_copy(part.at[m, grp], recv.at[me], b_recv).start()
                else:
                    send((grp + dp) % groups)
        else:
            each(groups - 1, lambda i: send((grp + i + 1) % groups))
            if k == 0:
                pltpu.make_async_copy(part.at[m, grp], recv.at[me], b_recv).start()
            else:
                send(grp)

    slot_f = slot_v[...].astype(F32)
    which = iota((slots, groups), 0)
    column_pick = jnp.zeros((slots, groups), F32)
    for k in range(per_peer):
        column_pick = jnp.where(which % per_peer == k, slot_f[k : k + 1, :], column_pick)
    column_pick = jnp.where(which // per_peer == iota((slots, groups), 1), column_pick, 0.0)
    target_col = jnp.sum(column_pick, axis=1, keepdims=True)
    i_id, j_id = iota((slots, slots), 0), iota((slots, slots), 1)
    target_row = jnp.sum(jnp.where(i_id == j_id, target_col, 0.0), axis=0, keepdims=True)
    same = target_col == target_row
    first_col = jnp.sum(jnp.where(same & (j_id < i_id), 1.0, 0.0), axis=1, keepdims=True) == 0.0
    first_row = jnp.sum(jnp.where(same & (i_id < j_id), 1.0, 0.0), axis=0, keepdims=True) == 0.0
    place_row = jnp.where(first_row, target_row, -1.0)
    packed[place_base : place_base + 1, :slots] = place_row
    same_w = jnp.where(same, 1.0, 0.0).astype(BF16)

    hits = []
    accum_col = jnp.zeros((slots, 1), F32)
    for t in range(tables):
        hit = target_col == (iota((slots, rows), 1) + t * rows).astype(F32)
        hits.append(hit)
        accum_col += jnp.sum(
            jnp.where(hit, accum_v[t : t + 1, :], 0.0), axis=1, keepdims=True
        )

    pltpu.make_async_copy(recv, recv, b_recv).wait()
    for g in range(groups):
        group_sum = recv[g * lanes].astype(F32)
        for q in range(1, lanes):
            group_sum += recv[g * lanes + q].astype(F32)
        incoming[g * per_peer : (g + 1) * per_peer, :] = group_sum
    grads = jnp.dot(same_w, incoming[...].astype(BF16), preferred_element_type=F32)
    square_col = jnp.sum(grads * grads, axis=1, keepdims=True) * (1.0 / embed)
    square_first = jnp.where(first_col, square_col, 0.0)
    local = embed * jnp.sum(square_first, axis=0, keepdims=True)
    norm_out[...] = jnp.broadcast_to(local, (1, 128))

    def tell(far):
        pltpu.make_async_remote_copy(
            src_ref=norm_out,
            dst_ref=norm_in.at[me],
            send_sem=c_send,
            recv_sem=c_recv,
            device_id=(far // lanes, far % lanes),
            device_id_type=MESH,
        ).start()

    if devices <= 64:
        for d in sorted(range(1, devices), key=lambda d: abs(d - devices // 2)):
            tell((me + d) % devices)
    else:
        each(devices - 1, lambda i: tell((me + i + 1) % devices))
    pltpu.make_async_copy(norm_out, norm_in.at[me], c_recv).start()

    square_rows = [
        jnp.sum(jnp.where(hit, square_first, 0.0), axis=0, keepdims=True) for hit in hits
    ]
    for copy in a_copies:
        copy.wait_send()
    sent = recv.at[pl.ds(0, devices - 1)]
    pltpu.make_async_copy(sent, sent, b_send).wait()

    pltpu.make_async_copy(norm_in, norm_in, c_recv).wait()
    norm_total = jnp.sum(norm_in[...], axis=0)[:, :1]
    clip_limit = 0.5 * math.sqrt(devices * slots * embed)
    clip = clip_limit / jnp.maximum(jnp.sqrt(norm_total), clip_limit)
    for t in range(tables):
        packed[accum_base + t : accum_base + t + 1, :rows] = accum_v[t : t + 1, :] + clip * clip * square_rows[t]
    new_accum_col = accum_col + clip * clip * square_col
    delta = LEARN_RATE * clip * grads / (jnp.sqrt(new_accum_col) + EPSILON)
    packed[:slots, :embed] = delta
    told = norm_in.at[pl.ds(0, devices - 1)]
    pltpu.make_async_copy(told, told, c_send).wait()


def update_kernel(
    chunk, slots, place_base, accum_base, weights, packed, wout, aout, held, accum, sems, accum_sem
):
    accum[...] = packed[accum_base : accum_base + accum.shape[0], : accum.shape[1]]
    accum_copy = pltpu.make_async_copy(accum, aout, accum_sem)
    accum_copy.start()
    delta = packed[:slots, : weights.shape[2]]
    high = delta.astype(BF16)
    deltas = jnp.concatenate([high, (delta - high.astype(F32)).astype(BF16)], axis=0)
    place_row = packed[place_base : place_base + 1, :slots]
    place_row = jnp.concatenate([place_row, place_row], axis=1)
    tables, rows = weights.shape[0], weights.shape[1]
    copies = []
    for t in range(tables):
        for c in range(0, rows, chunk):
            row_id = (iota((chunk, 1), 0) + (t * rows + c)).astype(F32)
            place = jnp.where(row_id == place_row, 1.0, 0.0).astype(BF16)
            held[t, c : c + chunk] = weights[t, c : c + chunk] - jnp.dot(
                place, deltas, preferred_element_type=F32
            )
            copies.append(
                pltpu.make_async_copy(
                    held.at[t, pl.ds(c, chunk)],
                    wout.at[t, pl.ds(c, chunk)],
                    sems.at[len(copies)],
                )
            )
            copies[-1].start()
    for copy in copies:
        copy.wait()
    accum_copy.wait()


def per_device(groups, lanes, grad_pooled, bag_len, lookup_slot, slot_row, weights, accum):
    batch, tables_all, embed = grad_pooled.shape
    samples, tables, depth = lookup_slot.shape
    rows = accum.shape[1]
    per_peer = slot_row.shape[3]
    devices = groups * lanes
    slots = groups * per_peer
    mark_type = BF16 if slots <= 256 else F32
    place_base = -(-slots // 8) * 8
    accum_base = place_base + 8
    packed_shape = (accum_base + -(-tables // 8) * 8, max(embed, rows, slots))
    anywhere = pl.BlockSpec(memory_space=pl.ANY)
    vmem = pl.BlockSpec(memory_space=pltpu.VMEM)
    packed = pl.pallas_call(
        functools.partial(kernel, groups, lanes, place_base, accum_base),
        out_shape=jax.ShapeDtypeStruct(packed_shape, F32),
        in_specs=[pl.BlockSpec(memory_space=pltpu.HBM)] * 5,
        out_specs=vmem,
        cost_estimate=pl.CostEstimate(
            flops=8 * slots * batch * tables_all * embed,
            bytes_accessed=32 * batch * tables_all * embed,
            transcendentals=0,
        ),
        scratch_shapes=[
            pltpu.VMEM((batch * tables_all, embed), BF16),
            pltpu.VMEM((embed // 128, batch * tables_all, 128), F32),
            pltpu.VMEM((tables_all, batch, embed), BF16),
            pltpu.VMEM((tables_all, batch), jnp.int32),
            pltpu.VMEM((lanes, tables, depth, batch), mark_type),
            pltpu.VMEM((lanes, tables, depth, batch), jnp.int32),
            pltpu.VMEM((lanes - 1, tables, depth, batch), mark_type),
            pltpu.VMEM((per_peer, groups), jnp.int32),
            pltpu.VMEM((tables, rows), F32),
            pltpu.VMEM((lanes, groups, per_peer, embed), BF16),
            pltpu.VMEM((devices, per_peer, embed), BF16),
            pltpu.VMEM((slots, embed), F32),
            pltpu.VMEM((1, 128), F32),
            pltpu.VMEM((devices, 1, 128), F32),
            pltpu.SemaphoreType.DMA((4,)),
            pltpu.SemaphoreType.DMA((lanes,)),
            pltpu.SemaphoreType.DMA((lanes - 1,)),
            pltpu.SemaphoreType.DMA((lanes - 1,)),
            pltpu.SemaphoreType.DMA,
            pltpu.SemaphoreType.DMA,
            pltpu.SemaphoreType.DMA,
            pltpu.SemaphoreType.DMA,
        ],
        compiler_params=pltpu.CompilerParams(
            collective_id=0, has_side_effects=True
        ),
    )(
        grad_pooled.reshape(batch * tables_all, embed),
        bag_len.T,
        jnp.transpose(lookup_slot, (1, 2, 0)),
        slot_row.reshape(groups, per_peer).T,
        accum,
    )
    chunk = min(rows, 128)
    return pl.pallas_call(
        functools.partial(update_kernel, chunk, slots, place_base, accum_base),
        out_shape=(
            jax.ShapeDtypeStruct(weights.shape, F32),
            jax.ShapeDtypeStruct(accum.shape, F32),
        ),
        in_specs=[vmem, vmem],
        out_specs=(anywhere, anywhere),
        scratch_shapes=[
            pltpu.VMEM(weights.shape, F32),
            pltpu.VMEM(accum.shape, F32),
            pltpu.SemaphoreType.DMA((tables * (rows // chunk),)),
            pltpu.SemaphoreType.DMA,
        ],
        compiler_params=pltpu.CompilerParams(vmem_limit_bytes=8 << 20),
    )(weights, packed)


def solution(mesh):
    placed = (
        P(("grp", "lane"), None, None),
        P(("grp", "lane"), None),
        P("grp", "lane", None),
        P("grp", "lane", None, None),
        P("lane", "grp", None),
        P("lane", "grp"),
    )
    return jax.shard_map(
        functools.partial(per_device, mesh.shape["grp"], mesh.shape["lane"]),
        mesh=mesh,
        in_specs=placed,
        out_specs=(P("lane", "grp", None), P("lane", "grp")),
        check_vma=False,
    )
```

```python
import functools
import math

import jax
import jax.numpy as jnp
from jax import lax
from jax.experimental import pallas as pl
from jax.experimental.pallas import tpu as pltpu
from jax.sharding import PartitionSpec as P

MESH = pl.DeviceIdType.MESH
LEARN_RATE = 0.3
EPSILON = 1e-06
F32 = jnp.float32
BF16 = jnp.bfloat16


def each(count, body):
    if count <= 64:
        for i in range(count):
            body(i)
    else:

        def step(i, carry):
            body(i)
            return carry

        lax.fori_loop(0, count, step, 0)


def iota(shape, dim):
    return lax.broadcasted_iota(jnp.int32, shape, dim)


def kernel(
    groups,
    lanes,
    place_base,
    accum_base,
    grad_hbm,
    len_hbm,
    look_hbm,
    slot_hbm,
    accum_hbm,
    packed,
    grad_in,
    grad_f32,
    grad_t,
    len_v,
    marks,
    marks_in,
    marks_out,
    slot_v,
    accum_v,
    part,
    recv,
    incoming,
    norm_out,
    norm_in,
    load_sem,
    look_sem,
    a_send,
    a_recv,
    b_send,
    b_recv,
    c_send,
    c_recv,
):
    devices = groups * lanes
    per_peer, embed = recv.shape[1], recv.shape[2]
    slots = groups * per_peer
    tables_all, batch = grad_t.shape[0], grad_t.shape[1]
    tables = tables_all // lanes
    depth = marks.shape[2]
    rows = accum_v.shape[1]
    grp = lax.axis_index("grp")
    lane = lax.axis_index("lane")
    me = grp * lanes + lane
    sign = 2 * (grp // (groups // 2)) - 1

    lane_steps = [(dx, dc) for dx in range(lanes // 2) for dc in range(2)]

    def lane_peer(step, sign):
        dx, dc = step
        half = lanes // 2
        chip = (lane // 2 + sign * dx + half) % half
        return chip * 2 + (lane % 2 + dc) % 2

    def partial_of(m):
        highs, lows = [], []
        for t in range(tables):
            mark = marks[m, t].astype(F32)
            count = jnp.zeros((slots, batch), F32)
            for j in range(depth):
                count += jnp.where(mark[j : j + 1, :] == number, 1.0, 0.0)
            length = len_v[pl.ds(m * tables + t, 1), :].astype(F32)
            factor = count / length
            high = factor.astype(BF16)
            highs.append(high)
            lows.append((factor - high.astype(F32)).astype(BF16))
        factors = jnp.concatenate(
            [jnp.concatenate(highs, axis=1), jnp.concatenate(lows, axis=1)], axis=0
        )
        values = grad_t[pl.ds(m * tables, tables)].reshape(tables * batch, embed)
        both = jnp.dot(factors, values, preferred_element_type=F32)
        return both[:slots] + both[slots:]

    barrier = pltpu.get_barrier_semaphore()

    def greet(i):
        far = (me + sign * (i + 1) + devices) % devices
        pl.semaphore_signal(
            barrier, inc=1, device_id=(far // lanes, far % lanes), device_id_type=MESH
        )

    look_copies = []
    for k, step in enumerate(lane_steps):
        q = lane_peer(step, 1)
        src = look_hbm.at[:, :, pl.ds(pl.multiple_of(q * batch, batch), batch)]
        look_copies.append(pltpu.make_async_copy(src, marks_in.at[k], look_sem.at[k]))
        look_copies[-1].start()
    grad_copy = pltpu.make_async_copy(grad_hbm, grad_in, load_sem.at[0])
    grad_copy.start()
    if devices <= 64:
        for i in range(devices - 1):
            greet(i)
    else:
        each(devices - 1, greet)
    small_copies = [
        pltpu.make_async_copy(len_hbm, len_v, load_sem.at[1]),
        pltpu.make_async_copy(slot_hbm, slot_v, load_sem.at[2]),
        pltpu.make_async_copy(accum_hbm, accum_v, load_sem.at[3]),
    ]
    for copy in small_copies:
        copy.start()
    for copy in look_copies:
        copy.wait()
    for k in range(1, lanes):
        marks_out[k - 1] = marks_in[k].astype(F32).astype(marks_out.dtype)
    pl.semaphore_wait(barrier, devices - 1)

    a_copies = []
    for k, step in enumerate(lane_steps[1:], 1):
        copy = pltpu.make_async_remote_copy(
            src_ref=marks_out.at[k - 1],
            dst_ref=marks.at[lane],
            send_sem=a_send.at[k - 1],
            recv_sem=a_recv.at[k - 1],
            device_id=(grp, lane_peer(step, 1)),
            device_id_type=MESH,
        )
        copy.start()
        a_copies.append(copy)

    grad_copy.wait()
    for c in range(embed // 128):
        grad_f32[c] = grad_in[:, c * 128 : (c + 1) * 128].astype(F32)
    for t in range(tables_all):
        for c in range(embed // 128):
            grad_t[t, :, c * 128 : (c + 1) * 128] = grad_f32[
                c, pl.ds(t, batch, stride=tables_all), :
            ].astype(BF16)
    for copy in small_copies:
        copy.wait()

    marks[lane] = marks_in[0].astype(F32).astype(marks.dtype)
    number = iota((slots, batch), 0).astype(F32)
    far_first = list(range(1, groups)) + [0]

    for k, step in enumerate(lane_steps):
        m = lane_peer(step, -1)
        if k > 0:
            a_copies[k - 1].wait_recv()
        total = partial_of(m)
        for p in range(groups):
            part[m, p] = total[p * per_peer : (p + 1) * per_peer].astype(BF16)

        def send(p):
            pltpu.make_async_remote_copy(
                src_ref=part.at[m, p],
                dst_ref=recv.at[me],
                send_sem=b_send,
                recv_sem=b_recv,
                device_id=(p, m),
                device_id_type=MESH,
            ).start()

        if groups <= 64:
            for dp in far_first:
                if k == 0 and dp == 0:
                    pltpu.make_async_copy(part.at[m, grp], recv.at[me], b_recv).start()
                else:
                    send((grp + sign * dp + groups) % groups)
        else:
            each(groups - 1, lambda i: send((grp + i + 1) % groups))
            if k == 0:
                pltpu.make_async_copy(part.at[m, grp], recv.at[me], b_recv).start()
            else:
                send(grp)

    slot_f = slot_v[...].astype(F32)
    which = iota((slots, groups), 0)
    column_pick = jnp.zeros((slots, groups), F32)
    for k in range(per_peer):
        column_pick = jnp.where(which % per_peer == k, slot_f[k : k + 1, :], column_pick)
    column_pick = jnp.where(which // per_peer == iota((slots, groups), 1), column_pick, 0.0)
    target_col = jnp.sum(column_pick, axis=1, keepdims=True)
    i_id, j_id = iota((slots, slots), 0), iota((slots, slots), 1)
    target_row = jnp.sum(jnp.where(i_id == j_id, target_col, 0.0), axis=0, keepdims=True)
    same = target_col == target_row
    first_col = jnp.sum(jnp.where(same & (j_id < i_id), 1.0, 0.0), axis=1, keepdims=True) == 0.0
    first_row = jnp.sum(jnp.where(same & (i_id < j_id), 1.0, 0.0), axis=0, keepdims=True) == 0.0
    place_row = jnp.where(first_row, target_row, -1.0)
    packed[place_base : place_base + 1, :slots] = place_row
    same_w = jnp.where(same, 1.0, 0.0).astype(BF16)

    hits = []
    accum_col = jnp.zeros((slots, 1), F32)
    for t in range(tables):
        hit = target_col == (iota((slots, rows), 1) + t * rows).astype(F32)
        hits.append(hit)
        accum_col += jnp.sum(
            jnp.where(hit, accum_v[t : t + 1, :], 0.0), axis=1, keepdims=True
        )

    pltpu.make_async_copy(recv, recv, b_recv).wait()
    for g in range(groups):
        group_sum = recv[g * lanes].astype(F32)
        for q in range(1, lanes):
            group_sum += recv[g * lanes + q].astype(F32)
        incoming[g * per_peer : (g + 1) * per_peer, :] = group_sum
    grads = jnp.dot(same_w, incoming[...].astype(BF16), preferred_element_type=F32)
    square_col = jnp.sum(grads * grads, axis=1, keepdims=True) * (1.0 / embed)
    square_first = jnp.where(first_col, square_col, 0.0)
    local = embed * jnp.sum(square_first, axis=0, keepdims=True)
    norm_out[...] = jnp.broadcast_to(local, (1, 128))

    def tell(far):
        pltpu.make_async_remote_copy(
            src_ref=norm_out,
            dst_ref=norm_in.at[me],
            send_sem=c_send,
            recv_sem=c_recv,
            device_id=(far // lanes, far % lanes),
            device_id_type=MESH,
        ).start()

    if devices <= 64:
        for d in range(1, devices):
            tell((me + sign * d + devices) % devices)
    else:
        each(devices - 1, lambda i: tell((me + i + 1) % devices))
    pltpu.make_async_copy(norm_out, norm_in.at[me], c_recv).start()

    square_rows = [
        jnp.sum(jnp.where(hit, square_first, 0.0), axis=0, keepdims=True) for hit in hits
    ]
    for copy in a_copies:
        copy.wait_send()
    sent = recv.at[pl.ds(0, devices - 1)]
    pltpu.make_async_copy(sent, sent, b_send).wait()

    pltpu.make_async_copy(norm_in, norm_in, c_recv).wait()
    norm_total = jnp.sum(norm_in[...], axis=0)[:, :1]
    clip_limit = 0.5 * math.sqrt(devices * slots * embed)
    clip = clip_limit / jnp.maximum(jnp.sqrt(norm_total), clip_limit)
    for t in range(tables):
        packed[accum_base + t : accum_base + t + 1, :rows] = accum_v[t : t + 1, :] + clip * clip * square_rows[t]
    new_accum_col = accum_col + clip * clip * square_col
    delta = LEARN_RATE * clip * grads / (jnp.sqrt(new_accum_col) + EPSILON)
    packed[:slots, :embed] = delta
    told = norm_in.at[pl.ds(0, devices - 1)]
    pltpu.make_async_copy(told, told, c_send).wait()


def update_kernel(
    chunk, slots, place_base, accum_base, weights, packed, wout, aout, held, accum, sems, accum_sem
):
    accum[...] = packed[accum_base : accum_base + accum.shape[0], : accum.shape[1]]
    accum_copy = pltpu.make_async_copy(accum, aout, accum_sem)
    accum_copy.start()
    delta = packed[:slots, : weights.shape[2]]
    high = delta.astype(BF16)
    deltas = jnp.concatenate([high, (delta - high.astype(F32)).astype(BF16)], axis=0)
    place_row = packed[place_base : place_base + 1, :slots]
    place_row = jnp.concatenate([place_row, place_row], axis=1)
    tables, rows = weights.shape[0], weights.shape[1]
    copies = []
    for t in range(tables):
        for c in range(0, rows, chunk):
            row_id = (iota((chunk, 1), 0) + (t * rows + c)).astype(F32)
            place = jnp.where(row_id == place_row, 1.0, 0.0).astype(BF16)
            held[t, c : c + chunk] = weights[t, c : c + chunk] - jnp.dot(
                place, deltas, preferred_element_type=F32
            )
            copies.append(
                pltpu.make_async_copy(
                    held.at[t, pl.ds(c, chunk)],
                    wout.at[t, pl.ds(c, chunk)],
                    sems.at[len(copies)],
                )
            )
            copies[-1].start()
    for copy in copies:
        copy.wait()
    accum_copy.wait()


def per_device(groups, lanes, grad_pooled, bag_len, lookup_slot, slot_row, weights, accum):
    batch, tables_all, embed = grad_pooled.shape
    samples, tables, depth = lookup_slot.shape
    rows = accum.shape[1]
    per_peer = slot_row.shape[3]
    devices = groups * lanes
    slots = groups * per_peer
    mark_type = BF16 if slots <= 256 else F32
    place_base = -(-slots // 8) * 8
    accum_base = place_base + 8
    packed_shape = (accum_base + -(-tables // 8) * 8, max(embed, rows, slots))
    anywhere = pl.BlockSpec(memory_space=pl.ANY)
    vmem = pl.BlockSpec(memory_space=pltpu.VMEM)
    packed = pl.pallas_call(
        functools.partial(kernel, groups, lanes, place_base, accum_base),
        out_shape=jax.ShapeDtypeStruct(packed_shape, F32),
        in_specs=[pl.BlockSpec(memory_space=pltpu.HBM)] * 5,
        out_specs=vmem,
        cost_estimate=pl.CostEstimate(
            flops=8 * slots * batch * tables_all * embed,
            bytes_accessed=32 * batch * tables_all * embed,
            transcendentals=0,
        ),
        scratch_shapes=[
            pltpu.VMEM((batch * tables_all, embed), BF16),
            pltpu.VMEM((embed // 128, batch * tables_all, 128), F32),
            pltpu.VMEM((tables_all, batch, embed), BF16),
            pltpu.VMEM((tables_all, batch), jnp.int32),
            pltpu.VMEM((lanes, tables, depth, batch), mark_type),
            pltpu.VMEM((lanes, tables, depth, batch), jnp.int32),
            pltpu.VMEM((lanes - 1, tables, depth, batch), mark_type),
            pltpu.VMEM((per_peer, groups), jnp.int32),
            pltpu.VMEM((tables, rows), F32),
            pltpu.VMEM((lanes, groups, per_peer, embed), BF16),
            pltpu.VMEM((devices, per_peer, embed), BF16),
            pltpu.VMEM((slots, embed), F32),
            pltpu.VMEM((1, 128), F32),
            pltpu.VMEM((devices, 1, 128), F32),
            pltpu.SemaphoreType.DMA((4,)),
            pltpu.SemaphoreType.DMA((lanes,)),
            pltpu.SemaphoreType.DMA((lanes - 1,)),
            pltpu.SemaphoreType.DMA((lanes - 1,)),
            pltpu.SemaphoreType.DMA,
            pltpu.SemaphoreType.DMA,
            pltpu.SemaphoreType.DMA,
            pltpu.SemaphoreType.DMA,
        ],
        compiler_params=pltpu.CompilerParams(
            collective_id=0, has_side_effects=True
        ),
    )(
        grad_pooled.reshape(batch * tables_all, embed),
        bag_len.T,
        jnp.transpose(lookup_slot, (1, 2, 0)),
        slot_row.reshape(groups, per_peer).T,
        accum,
    )
    chunk = min(rows, 128)
    return pl.pallas_call(
        functools.partial(update_kernel, chunk, slots, place_base, accum_base),
        out_shape=(
            jax.ShapeDtypeStruct(weights.shape, F32),
            jax.ShapeDtypeStruct(accum.shape, F32),
        ),
        in_specs=[vmem, vmem],
        out_specs=(anywhere, anywhere),
        scratch_shapes=[
            pltpu.VMEM(weights.shape, F32),
            pltpu.VMEM(accum.shape, F32),
            pltpu.SemaphoreType.DMA((tables * (rows // chunk),)),
            pltpu.SemaphoreType.DMA,
        ],
        compiler_params=pltpu.CompilerParams(vmem_limit_bytes=8 << 20),
    )(weights, packed)


def solution(mesh):
    placed = (
        P(("grp", "lane"), None, None),
        P(("grp", "lane"), None),
        P("grp", "lane", None),
        P("grp", "lane", None, None),
        P("lane", "grp", None),
        P("lane", "grp"),
    )
    return jax.shard_map(
        functools.partial(per_device, mesh.shape["grp"], mesh.shape["lane"]),
        mesh=mesh,
        in_specs=placed,
        out_specs=(P("lane", "grp", None), P("lane", "grp")),
        check_vma=False,
    )
```
